32 devices in a mesh: user: 8 (over z, x), pos: 4 (over y, core).
Axes of the slice: x: 2, y: 2, z: 4, core: 2. Of those that a mesh axis runs over, the one named last changes fastest.
Arguments:
- events: bfloat16 [8192, 256], P('user'), may hold values from -6 to 6
- owners: int32 [8192], P('user'), may hold values from 0 to 15, as said below
- offsets: int32 [8192], P('user'), may hold values from 0 to 2047, as said below
- w_key: bfloat16 [256, 256], replicated, may hold values from -0.375 to 0.375
- w_value: bfloat16 [256, 256], replicated, may hold values from -0.375 to 0.375
- cache_keys: bfloat16 [16, 6144, 256], P('user', 'pos'), may hold values from -7 to 7
- cache_values: bfloat16 [16, 6144, 256], P('user', 'pos'), may hold values from -6 to 6
- hist_len: int32 [16], P('user'), may hold values from 8 to 4096
- active: int32 [16], P('user'), may hold values 0 or 1
- candidates: bfloat16 [16, 1024, 256], P('user', 'pos'), may hold values from -100 to 100
Outputs:
- new_keys: bfloat16 [16, 6144, 256], P('user', 'pos')
- new_values: bfloat16 [16, 6144, 256], P('user', 'pos')
- attended: bfloat16 [16, 1024, 256], P('user', 'pos')
The draws below stay inside these ranges and needn't reach their ends.
Inputs may be any that keep to these rules, and one draw needn't show every extreme that they name: Among the events of one aligned block of 1024 (one index of user), at most 256 have owners among the users t * 2 to t * 2 + 1, for every t; in every draw some t receives exactly 256 from every block, and all those events belong to one user of that t. offsets[e] is the number of events before e, in the order of the array, that have the same owner as e.
All inputs are finite; a program needn't handle non-finite values. No bound on the sum of `active` on one device may be relied on, other than what follows from the above.
Results may differ from the reference program's by a relative error of at most 0.0067.
Values may be sent and summed in bfloat16 or wider, within the bound.
A program may use at most 128 MiB of HBM per device.

```python
import jax
import jax.numpy as jnp
from jax import lax

U_DEV = 2
P_DEV = 1536
EV_DEV = 1024
D = 256
F = 256
CAND = 1024
USERS = 16
HIST = 6144
EVENTS = 8192
CAP = 256
N_POS = 4


def key_head(key):
    head = jnp.clip(jax.random.normal(jax.random.fold_in(key, 7002), (USERS, 6, D), jnp.float32), -6.0, 6.0)
    return head


def draw_cache_keys(key, part):
    rows = jnp.clip(jax.random.normal(jax.random.fold_in(key, 7001), (USERS, HIST, D), jnp.float32), -6.0, 6.0)
    head = key_head(key)
    rows = rows.at[:, :6].set(head)
    return rows.astype(jnp.bfloat16)


def draw_candidates(key, part):
    values = jnp.clip(jax.random.normal(jax.random.fold_in(key, 7003), (USERS, CAND, D), jnp.float32), -6.0, 6.0)
    return values.astype(jnp.bfloat16)


def routing(key):
    groups = USERS // U_DEV
    width = groups * CAP
    splits = jax.random.split(jax.random.fold_in(key, 7101), groups)

    def shuffle(single):
        return jax.random.permutation(single, width).astype(jnp.int32)
    perms = jax.vmap(shuffle)(splits)
    full = jax.random.randint(jax.random.fold_in(key, 7102), (), 0, groups).astype(jnp.int32)
    column = jnp.arange(width, dtype=jnp.int32) // CAP
    score = jnp.where(column[None, :] == full, perms - width, perms)
    chosen = jnp.argsort(score, axis=1)[:, :EV_DEV].astype(jnp.int32)
    dest = chosen // CAP
    local = jax.random.randint(jax.random.fold_in(key, 7103), (groups, EV_DEV), 0, U_DEV).astype(jnp.int32)
    heavy = jax.random.randint(jax.random.fold_in(key, 7104), (), 0, U_DEV).astype(jnp.int32)
    local = jnp.where(dest == full, heavy, local).astype(jnp.int32)
    owners = (dest * U_DEV + local).reshape(-1).astype(jnp.int32)
    order_all = jnp.argsort(owners, stable=True).astype(jnp.int32)
    sorted_owner = owners[order_all]
    start = jnp.searchsorted(sorted_owner, sorted_owner, side='left').astype(jnp.int32)
    rank_sorted = jnp.arange(EVENTS, dtype=jnp.int32) - start
    offsets = jnp.zeros((EVENTS,), jnp.int32).at[order_all].set(rank_sorted)
    return (owners, offsets)


def draw_owners(key, part):
    return routing(key)[0]


def draw_offsets(key, part):
    return routing(key)[1]


def touch_ends(result, key, low, top_value):
    longest = result.shape.index(max(result.shape))
    spots = []
    for shift in (0, 1):
        where = [jax.random.randint(jax.random.fold_in(key, axis), (), 0, length) for axis, length in enumerate(result.shape)]
        where[longest] = (where[longest] + shift) % result.shape[longest]
        spots.append(tuple(where))
    return result.at[spots[0]].set(low).at[spots[1]].set(top_value)


def block_scale(rng, extent, cuts, low, top_value):
    def one(dim, blocks):
        steps = jax.random.uniform(jax.random.fold_in(jax.random.fold_in(rng, 6), dim), (blocks,), jnp.float32, low / len(cuts), top_value / len(cuts))
        return jnp.repeat(jnp.exp(steps), extent[dim] // blocks).reshape((-1,) + (1,) * (len(extent) - dim - 1))

    loudness = one(*cuts[0])
    for cut in cuts[1:]:
        loudness = loudness * one(*cut)
    return loudness


def normal_values(rng, extent, spread, limit, pieces=(), kind=jnp.bfloat16):
    loudness = block_scale(rng, extent, pieces, -0.22, 0.18) if pieces else 1.0
    values = jax.random.normal(rng, extent, jnp.float32) * spread * loudness
    return jnp.minimum(jnp.maximum(values, -limit), limit).astype(kind)


def setup_inputs(seed: int = 0) -> dict:
    key_list = jax.random.split(jax.random.key(seed), 11)
    return {
        "events": normal_values(key_list[0], (EVENTS, F), 1.0, 6.0, ((0, 8),)),
        "owners": draw_owners(jax.random.fold_in(key_list[10], 71), 0),
        "offsets": draw_offsets(jax.random.fold_in(key_list[10], 71), 0),
        "w_key": normal_values(key_list[3], (F, D), F ** -0.5, 0.375),
        "w_value": normal_values(key_list[4], (F, D), F ** -0.5, 0.375),
        "cache_keys": draw_cache_keys(jax.random.fold_in(key_list[10], 71), 0),
        "cache_values": normal_values(key_list[6], (USERS, HIST, D), 1.0, 6.0, ((0, 8), (1, 4))),
        "hist_len": touch_ends(jax.random.randint(key_list[7], (USERS,), 8, HIST - 2 * EV_DEV + 1), jax.random.fold_in(key_list[7], 1), 8, HIST - 2 * EV_DEV).astype(jnp.int32),
        "active": touch_ends((jax.random.randint(key_list[8], (USERS,), 0, 4) < 3).astype(jnp.int32), jax.random.fold_in(key_list[8], 1), 0, 1),
        "candidates": draw_candidates(jax.random.fold_in(key_list[10], 71), 0),
    }


def reference(events, owners, offsets, w_key, w_value, cache_keys, cache_values, hist_len, active, candidates):
    new_k = jnp.dot(events, w_key, preferred_element_type=jnp.float32).astype(jnp.bfloat16)
    new_v = jnp.dot(events, w_value, preferred_element_type=jnp.float32).astype(jnp.bfloat16)
    target = (hist_len[owners] + offsets).astype(jnp.int32)
    new_keys = cache_keys.at[owners, target].set(new_k)
    new_values = cache_values.at[owners, target].set(new_v)
    counts = jax.ops.segment_sum(jnp.ones_like(owners), owners, num_segments=USERS).astype(jnp.int32)
    limits = (hist_len + counts).astype(jnp.int32)
    scale = D ** -0.5

    def per_user(pack):
        query, key_rows, value_rows, bound, flag = pack
        scores = jnp.dot(query, key_rows.T, preferred_element_type=jnp.float32) * scale
        scores = scores.reshape(CAND, N_POS, P_DEV)
        position = jnp.arange(HIST, dtype=jnp.int32).reshape(N_POS, P_DEV)
        valid = (position < bound)[None]
        masked = jnp.where(valid, scores, jnp.float32(-1e30))
        block_max = jnp.max(masked, axis=2)
        expo = jnp.where(valid, jnp.exp(masked - block_max[:, :, None]), jnp.float32(0.0))
        block_sum = jnp.sum(expo, axis=2)
        weights = expo.astype(jnp.bfloat16)
        parts = jnp.einsum("cbp,bpd->cbd", weights.astype(jnp.float32),
                           value_rows.reshape(N_POS, P_DEV, D).astype(jnp.float32))
        top = jnp.max(block_max, axis=1)
        factor = jnp.exp(block_max - top[:, None])
        total = jnp.sum(block_sum * factor, axis=1)
        acc = jnp.sum(parts * factor[:, :, None], axis=1)
        return (acc / total[:, None] * flag).astype(jnp.bfloat16)

    attended = lax.map(per_user, (candidates, new_keys, new_values, limits, active.astype(jnp.float32)))
    return new_keys, new_values, attended
```

```python
import functools
import math

import jax
import jax.numpy as jnp
from jax import lax
from jax.experimental import pallas as pl
from jax.experimental.pallas import tpu as pltpu
from jax.sharding import PartitionSpec as P

MESH = pl.DeviceIdType.MESH
NT = (((1,), (1,)), ((), ()))
TAIL = 16
STEP = 64


def pos_peers():
    p = lax.axis_index("pos")
    near = p + 1 - 2 * lax.rem(p, 2)
    far = lax.rem(p + 2, 4)
    return p, near, far


def merged_kernel(
    groups, users_here, cap, scale,
    owners_ref, hist_ref, active_ref, events_hbm, cand_hbm, keys_hbm, values_hbm,
    w_key_hbm, w_value_hbm,
    fresh_ref, counts_ref, out_ref, keys_ref, values_ref,
    events_ref, queries, weight_ref, rows_ref, packed, flipped, eye,
    acc, stat, near_out, near_part, near_stat, far_out, far_stat_out, far_part, far_stat,
    load_sem, a2a_send, a2a_recv, hop_send, hop_recv, q_send, q_recv,
    near_send, near_recv, far_send, far_recv,
):
    me = lax.axis_index("user")
    p, near, far = pos_peers()
    low, high = lax.rem(p, 2), p // 2
    cross = 2 * (1 - high) + 1 - low
    half = groups // 2

    def partner(k, odd):
        bit = lax.rem(me, 2)
        there = me + odd * (1 - 2 * bit)
        for n in range(1, groups.bit_length() - 1):
            if (2 * k >> n) % 2:
                there += (1 - 2 * lax.rem(me // 2**n, 2)) * 2**n
        return there

    peers = [partner(k, low) for k in range(half)]
    near_sources = [partner(k, 1 - low) for k in range(half)]
    sends = list(range(half))[::-1]
    block_rows, width = keys_ref.shape[1:]
    quarter = queries.shape[2]

    def load(src, dst, n):
        copy = pltpu.make_async_copy(src, dst, load_sem.at[n])
        copy.start()
        return copy

    events_in = load(events_hbm, events_ref, 0)
    own_q = load(cand_hbm, queries.at[p], 1)
    keys_in = load(keys_hbm, keys_ref, 2)
    values_in = load(values_hbm, values_ref, 3)
    weights_in = [load(w_key_hbm, weight_ref.at[0], 4), load(w_value_hbm, weight_ref.at[1], 5)]

    barrier = pltpu.get_barrier_semaphore()
    for peer in (near, far):
        pl.semaphore_signal(barrier, inc=1, device_id={"pos": peer}, device_id_type=MESH)
    for peer in peers:
        @pl.when(peer != me)
        def _():
            pl.semaphore_signal(barrier, inc=1, device_id={"user": peer}, device_id_type=MESH)

    per_event = events_ref.shape[0]
    features = events_ref.shape[1]
    users = groups * users_here
    owner = owners_ref[...]
    user_id = lax.broadcasted_iota(jnp.int32, (users, per_event), 0)
    same = (user_id == owner).astype(jnp.float32)
    before = (
        lax.broadcasted_iota(jnp.int32, (per_event, per_event), 0)
        <= lax.broadcasted_iota(jnp.int32, (per_event, per_event), 1)
    ).astype(jnp.float32).astype(jnp.bfloat16)
    ranks = jnp.dot(same.astype(jnp.bfloat16), before, preferred_element_type=jnp.float32)
    counts = jnp.sum(same, axis=1, keepdims=True)
    dest = owner // users_here
    earlier = (user_id >= dest * users_here) & (user_id < owner)
    slot = jnp.sum(jnp.where(earlier, counts, 0.0) + same * ranks, axis=0, keepdims=True) - 1.0
    slot = slot.astype(jnp.int32)
    slot_id = lax.broadcasted_iota(jnp.int32, (cap, per_event), 0)
    lane = lax.broadcasted_iota(jnp.int32, (users, features), 1)
    lane_user = lax.broadcasted_iota(jnp.int32, (users, features), 0)

    def hop(ref_src, ref_dst, send, recv, peer):
        return pltpu.make_async_remote_copy(
            src_ref=ref_src, dst_ref=ref_dst, send_sem=send, recv_sem=recv,
            device_id={"pos": peer}, device_id_type=MESH,
        )

    def q_hop(n, c, u, peer):
        return hop(queries.at[c, u], queries.at[c, u], q_send.at[n, u], q_recv.at[n, u], peer)

    def a2a(k):
        return pltpu.make_async_remote_copy(
            src_ref=packed.at[k], dst_ref=rows_ref.at[me],
            send_sem=a2a_send.at[k], recv_sem=a2a_recv.at[k],
            device_id={"user": peers[k]}, device_id_type=MESH,
        )

    def own(k):
        return pltpu.make_async_copy(packed.at[k], rows_ref.at[me], load_sem.at[6])

    def pack(k):
        peer = peers[k]
        wanted = jnp.where(dest == peer, slot, -1)
        pick = (wanted == slot_id).astype(jnp.float32).astype(jnp.bfloat16)
        packed[k, :cap, :] = jnp.dot(
            pick, events_ref[...], preferred_element_type=jnp.float32
        ).astype(jnp.bfloat16)
        row = jnp.sum(
            jnp.where(lane_user == lane + peer * users_here, counts, 0.0), axis=0, keepdims=True
        )
        packed[k, cap:, :] = jnp.broadcast_to(row, (TAIL, features)).astype(jnp.bfloat16)

    def post(k):
        @pl.when(peers[k] != me)
        def _():
            a2a(k).start()

        if k == 0:
            @pl.when(peers[k] == me)
            def _():
                own(k).start()

    def arrive(k):
        @pl.when(peers[k] != me)
        def _():
            a2a(k).wait_recv()

        if k == 0:
            @pl.when(peers[k] == me)
            def _():
                own(k).wait()

        forward(k, peers[k]).start()

    def forward(k, source):
        block = rows_ref.at[source]
        return hop(block, block, hop_send.at[k], hop_recv.at[k], near)

    events_in.wait()
    early = half // 2
    for k in sends[:early]:
        pack(k)
    own_q.wait()
    pl.semaphore_wait(barrier, 1 + half + low)
    for u in range(users_here):
        q_hop(0, p, u, far).start()
    for u in range(users_here):
        q_hop(1, p, u, near).start()
    for k in sends[:early]:
        post(k)
    for k in sends[early:]:
        pack(k)
        post(k)

    eye[...] = (
        lax.broadcasted_iota(jnp.int32, (width, width), 0)
        == lax.broadcasted_iota(jnp.int32, (width, width), 1)
    ).astype(jnp.float32).astype(jnp.bfloat16)
    factor = scale * math.log2(math.e)
    position = lax.broadcasted_iota(jnp.int32, (block_rows, quarter), 0) + p * block_rows
    keys_in.wait()
    values_in.wait()

    def flip(rows):
        return lax.dot_general(
            eye[...], rows, NT, preferred_element_type=jnp.float32
        ).astype(jnp.bfloat16)

    for u in range(users_here):
        flipped[u] = flip(values_ref[u])

    def two_rows(top, total):
        return jnp.concatenate(
            [jnp.broadcast_to(top, (4, quarter)), jnp.broadcast_to(total, (4, quarter))], axis=0
        )

    def weigh(scores, floor):
        top = jnp.maximum(jnp.max(scores, axis=0, keepdims=True) * factor, floor)
        expo = jnp.exp2(scores * factor - top)
        return top, jnp.sum(expo, axis=0, keepdims=True), expo.astype(jnp.bfloat16)

    def copies(pairs, send, recv, n, peer):
        return [
            hop(src, dst, send.at[i, n], recv.at[i, n], peer)
            for i, (src, dst) in enumerate(pairs)
        ]

    def near_copies(n, u):
        return copies(
            (
                (near_out.at[n, u], near_part.at[n, u]),
                (stat.at[2 + n, u], near_stat.at[n, u]),
            ),
            near_send, near_recv, n * users_here + u, near,
        )

    def far_copies(u):
        return copies(
            ((far_out.at[u], far_part.at[u]), (far_stat_out.at[u], far_stat.at[u])),
            far_send, far_recv, u, far,
        )

    def merge(top, total, part, other, other_part):
        new_top = jnp.maximum(top, other[0:1])
        mine = jnp.exp2(top - new_top)
        theirs = jnp.exp2(other[0:1] - new_top)
        total = total * mine + other[4:5] * theirs
        return new_top, total, part * mine + other_part.astype(jnp.float32) * theirs

    def send_far(u):
        for copy in near_copies(1, u):
            copy.wait_recv()
        old = stat[1, u]
        top, total, part = merge(
            old[0:1], old[4:5], acc[1, u], near_stat[1, u], near_part[1, u]
        )
        far_out[u] = part.astype(jnp.bfloat16)
        far_stat_out[u] = two_rows(top, total)
        for copy in far_copies(u):
            copy.start()

    chunk = (p, far, near, cross)

    def ready(kind, u):
        if kind == 2:
            q_hop(1, near, u, near).wait_recv()
        if kind == 1:
            q_hop(0, far, u, far).wait_recv()
            q_hop(2, far, u, near).start()
        if kind == 3:
            q_hop(2, cross, u, near).wait_recv()

    def finish(kind, u, scores):
        top, total, weights = weigh(jnp.where(position < hist_ref[u], scores, -1e33), -1e29)
        part = jnp.dot(flipped[u], weights, preferred_element_type=jnp.float32)
        stat[kind, u] = two_rows(top, total)
        if kind < 2:
            acc[kind, u] = part
        else:
            near_out[kind - 2, u] = part.astype(jnp.bfloat16)
            for copy in near_copies(kind - 2, u):
                copy.start()
        if kind == 1 and u > 0:
            send_far(u - 1)

    items = [(0, u) for u in range(users_here)]
    for u in range(users_here):
        items += [(2, u), (1, u), (3, u)]
    last = None
    for kind, u in items:
        ready(kind, u)
        scores = lax.dot_general(
            keys_ref[u], queries[chunk[kind], u], NT, preferred_element_type=jnp.float32
        )
        if last is not None:
            finish(*last)
        last = (kind, u, scores)
    finish(*last)
    send_far(users_here - 1)
    for u in range(users_here):
        for copy in near_copies(0, u):
            copy.wait_recv()
        old = stat[0, u]
        top, total, part = merge(
            old[0:1], old[4:5], acc[0, u], near_stat[0, u], near_part[0, u]
        )
        acc[0, u] = part
        stat[0, u] = two_rows(top, total)
    for copy in weights_in:
        copy.wait()

    slots = lax.broadcasted_iota(jnp.int32, (cap, quarter), 0).astype(jnp.float32)

    def project(source):
        raw = rows_ref[source, :cap, :]
        row = pl.multiple_of(STEP + source * cap, 8)
        made = []
        for i in range(2):
            product = jnp.dot(raw, weight_ref[i], preferred_element_type=jnp.float32)
            product = product.astype(jnp.bfloat16)
            made.append(product)
            for n in range(width // 128):
                fresh_ref[i * (width // 128) + n, pl.ds(row, cap)] = product[
                    :, n * 128 : n * 128 + 128
                ].astype(jnp.float32)
        tail = rows_ref[source, cap:, :].astype(jnp.float32)
        begin = jnp.zeros((1, 1), jnp.float32)
        mask = []
        for u in range(users_here):
            end = begin + tail[0:1, u : u + 1]
            mask.append((slots >= begin) & (slots < end))
            begin = end
        return made[0], flip(made[1]), mask

    def fresh(sources):
        blocks = [project(source) for source in sources]
        keys_new = jnp.concatenate([b[0] for b in blocks], axis=0)
        flipped_new = jnp.concatenate([b[1] for b in blocks], axis=1)
        scores = [
            lax.dot_general(keys_new, queries[p, u], NT, preferred_element_type=jnp.float32)
            for u in range(users_here)
        ]
        for u in range(users_here):
            mask = jnp.concatenate([b[2][u] for b in blocks], axis=0)
            old = stat[0, u]
            top, total, weights = weigh(jnp.where(mask, scores[u], -1e33), old[0:1])
            shrink = jnp.exp2(old[0:1] - top)
            acc[0, u] = acc[0, u] * shrink + jnp.dot(
                flipped_new, weights, preferred_element_type=jnp.float32
            )
            stat[0, u] = two_rows(top, total + old[4:5] * shrink)

    soon = range(half // 2)
    late = range(half // 2, half)
    for k in soon:
        arrive(k)
    for k in soon:
        forward(k, near_sources[k]).wait_recv()
    fresh([source for k in soon for source in (peers[k], near_sources[k])])
    for k in late:
        arrive(k)
    fresh([peers[k] for k in late])
    for k in late:
        forward(k, near_sources[k]).wait_recv()
    fresh([near_sources[k] for k in late])
    for g in range(groups):
        counts_ref[g : g + 1, :] = rows_ref[g, cap : cap + TAIL, :128].astype(jnp.float32)[
            0:1
        ].astype(jnp.int32)

    for u in range(users_here):
        for copy in far_copies(u):
            copy.wait_recv()
        mine = stat[0, u]
        top, total, part = merge(mine[0:1], mine[4:5], acc[0, u], far_stat[u], far_part[u])
        flag = active_ref[u].astype(jnp.float32)
        out_ref[u] = (part * (flag / total)).T.astype(jnp.bfloat16)
    for u in range(users_here):
        q_hop(0, p, u, far).wait_send()
        q_hop(1, p, u, near).wait_send()
        q_hop(2, far, u, near).wait_send()
        for n in range(2):
            for copy in near_copies(n, u):
                copy.wait_send()
        for copy in far_copies(u):
            copy.wait_send()
    for k in range(half):
        @pl.when(peers[k] != me)
        def _():
            a2a(k).wait_send()

        forward(k, peers[k]).wait_send()


def place_kernel(
    groups, cap,
    count_ref, hist_ref, made_ref, keys_ref, values_ref, attended_ref,
    new_keys_hbm, new_values_hbm, out_hbm,
    cache, out_sem, read_sem,
):
    users_here, rows, width = keys_ref.shape
    sources = (keys_ref, values_ref)
    targets = (new_keys_hbm, new_values_hbm)
    origin = lax.axis_index("pos") * rows
    read = pltpu.make_async_copy(attended_ref, out_hbm, read_sem)
    read.start()

    def leave(u, i, source):
        return pltpu.make_async_copy(source, targets[i].at[u], out_sem.at[u, i])

    begin = [hist_ref[u] - origin for u in range(users_here)]
    end = [
        lax.fori_loop(0, groups, lambda g, n, u=u: n + count_ref[g, u], begin[u])
        for u in range(users_here)
    ]
    touched = [
        (begin[u] < rows) & (end[u] > 0) & (end[u] > begin[u]) for u in range(users_here)
    ]
    for u in range(users_here):
        @pl.when(jnp.logical_not(touched[u]))
        def _():
            for i in range(2):
                leave(u, i, sources[i].at[u]).start()

    row = lax.broadcasted_iota(jnp.int32, (STEP, 128), 0)
    for u in range(users_here):
        @pl.when(touched[u])
        def _():
            for i in range(2):
                cache[u, i] = sources[i][u]

            def place(g, at):
                size = count_ref[g, u]

                @pl.when((size > 0) & (at < rows) & (at + size > 0))
                def _():
                    low = lax.fori_loop(0, u, lambda v, n: n + count_ref[g, v], 0)
                    first = jnp.maximum(at, 0) // 16 * 16
                    last = jnp.minimum(at + size, rows)

                    def blend(n, carry):
                        to = pl.multiple_of(jnp.minimum(first + n * STEP, rows - STEP), 16)
                        start = STEP + g * cap + low + to - at
                        inside = (row >= at - to) & (row < at + size - to)
                        for i in range(2):
                            for tile in range(width // 128):
                                lanes = slice(tile * 128, tile * 128 + 128)
                                fresh = made_ref[i * (width // 128) + tile, pl.ds(start, STEP), :]
                                old = cache[u, i, pl.ds(to, STEP), lanes].astype(jnp.float32)
                                cache[u, i, pl.ds(to, STEP), lanes] = jnp.where(
                                    inside, fresh, old
                                ).astype(jnp.bfloat16)
                        return carry

                    lax.fori_loop(0, (last - first + STEP - 1) // STEP, blend, 0)

                return at + size

            lax.fori_loop(0, groups, place, begin[u])
            for i in range(2):
                leave(u, i, cache.at[u, i]).start()

    for u in range(users_here):
        for i in range(2):
            leave(u, i, sources[i].at[u]).wait()
    read.wait()


def on_device(
    events, owners, offsets, w_key, w_value, cache_keys, cache_values, hist_len, active, candidates
):
    groups = lax.axis_size("user")
    blocks = lax.axis_size("pos")
    users_here, block_rows, width = cache_keys.shape
    per_event, features = events.shape
    cap = 2 * per_event // groups
    quarter = candidates.shape[1]
    half = groups // 2
    vmem = pl.BlockSpec(memory_space=pltpu.VMEM)
    smem = pl.BlockSpec(memory_space=pltpu.SMEM)
    hbm = pl.BlockSpec(memory_space=pltpu.HBM)
    dma = pltpu.SemaphoreType.DMA
    bf16, f32 = jnp.bfloat16, jnp.float32

    made, counts, attended, keys, values = pl.pallas_call(
        functools.partial(merged_kernel, groups, users_here, cap, width ** -0.5),
        out_shape=(
            jax.ShapeDtypeStruct((width // 64, groups * cap + 2 * STEP, 128), f32),
            jax.ShapeDtypeStruct((groups, 128), jnp.int32),
            jax.ShapeDtypeStruct(candidates.shape, bf16),
            jax.ShapeDtypeStruct(cache_keys.shape, bf16),
            jax.ShapeDtypeStruct(cache_values.shape, bf16),
        ),
        in_specs=[vmem, smem, smem] + [hbm] * 6,
        out_specs=(vmem,) * 5,
        scratch_shapes=[
            pltpu.VMEM(events.shape, bf16),
            pltpu.VMEM((blocks,) + candidates.shape, bf16),
            pltpu.VMEM((2, features, width), bf16),
            pltpu.VMEM((groups, cap + TAIL, features), bf16),
            pltpu.VMEM((half, cap + TAIL, features), bf16),
            pltpu.VMEM((users_here, width, block_rows), bf16),
            pltpu.VMEM((width, width), bf16),
            pltpu.VMEM((2, users_here, width, quarter), f32),
            pltpu.VMEM((4, users_here, 8, quarter), f32),
            pltpu.VMEM((2, users_here, width, quarter), bf16),
            pltpu.VMEM((2, users_here, width, quarter), bf16),
            pltpu.VMEM((2, users_here, 8, quarter), f32),
            pltpu.VMEM((users_here, width, quarter), bf16),
            pltpu.VMEM((users_here, 8, quarter), f32),
            pltpu.VMEM((users_here, width, quarter), bf16),
            pltpu.VMEM((users_here, 8, quarter), f32),
            dma((7,)), dma((half,)), dma((half,)), dma((half,)), dma((half,)),
            dma((3, users_here)), dma((3, users_here)),
            dma((2, 2 * users_here)), dma((2, 2 * users_here)),
            dma((2, users_here)), dma((2, users_here)),
        ],
        compiler_params=pltpu.CompilerParams(
            collective_id=0, has_side_effects=True, vmem_limit_bytes=28 * 2**20
        ),
        name="merged",
    )(
        *[
            pltpu.with_memory_space_constraint(x, pltpu.HBM)
            for x in (
                owners.reshape(1, per_event), hist_len, active, events, candidates,
                cache_keys, cache_values, w_key, w_value,
            )
        ]
    )

    return pl.pallas_call(
        functools.partial(place_kernel, groups, cap),
        out_shape=(
            jax.ShapeDtypeStruct(cache_keys.shape, bf16),
            jax.ShapeDtypeStruct(cache_values.shape, bf16),
            jax.ShapeDtypeStruct(candidates.shape, bf16),
        ),
        in_specs=[smem, smem] + [vmem] * 4,
        out_specs=(hbm,) * 3,
        scratch_shapes=[
            pltpu.VMEM((users_here, 2, block_rows, width), bf16),
            dma((users_here, 2)), dma,
        ],
        compiler_params=pltpu.CompilerParams(vmem_limit_bytes=28 * 2**20),
        name="place",
    )(counts, hist_len, made, keys, values, attended)


def solution(mesh):
    placed = (
        P("user", None),
        P("user"),
        P("user"),
        P(),
        P(),
        P("user", "pos", None),
        P("user", "pos", None),
        P("user"),
        P("user"),
        P("user", "pos", None),
    )
    return jax.shard_map(
        on_device,
        mesh=mesh,
        in_specs=placed,
        out_specs=(P("user", "pos", None), P("user", "pos", None), P("user", "pos", None)),
        check_vma=False,
    )
```

```python
import functools
import math

import jax
import jax.numpy as jnp
from jax import lax
from jax.experimental import pallas as pl
from jax.experimental.pallas import tpu as pltpu
from jax.sharding import PartitionSpec as P

MESH = pl.DeviceIdType.MESH
NT = (((1,), (1,)), ((), ()))
TAIL = 16
STEP = 64


def pos_peers():
    p = lax.axis_index("pos")
    near = p + 1 - 2 * lax.rem(p, 2)
    far = lax.rem(p + 2, 4)
    return p, near, far


def merged_kernel(
    groups, users_here, cap, scale,
    owners_hbm, hist_hbm, active_hbm, events_hbm, cand_hbm, keys_hbm, values_hbm,
    w_key_hbm, w_value_hbm,
    fresh_ref, counts_ref, out_ref, keys_ref, values_ref,
    owners_ref, hist_ref, active_ref, events_ref, queries, weight_ref, rows_ref, packed, flipped, eye, turned_weight,
    acc, stat, near_out, near_part, near_stat, far_out, far_stat_out, far_part, far_stat,
    load_sem, a2a_send, a2a_recv, hop_send, hop_recv, q_send, q_recv,
    near_send, near_recv, far_send, far_recv,
):
    me = lax.axis_index("user")
    p, near, far = pos_peers()
    low, high = lax.rem(p, 2), p // 2
    cross = 2 * (1 - high) + 1 - low
    half = groups // 2

    def partner(k, odd):
        bit = lax.rem(me, 2)
        there = me + odd * (1 - 2 * bit)
        for n in range(1, groups.bit_length() - 1):
            if (2 * k >> n) % 2:
                there += (1 - 2 * lax.rem(me // 2**n, 2)) * 2**n
        return there

    peers = [partner(k, low) for k in range(half)]
    near_sources = [partner(k, 1 - low) for k in range(half)]
    soon, mid, late = range(half // 2), range(half // 2, 3 * half // 4), range(3 * half // 4, half)
    block_rows, width = keys_ref.shape[1:]
    quarter = queries.shape[2]

    def load(src, dst, n):
        copy = pltpu.make_async_copy(src, dst, load_sem.at[n])
        copy.start()
        return copy

    owners_in = load(owners_hbm, owners_ref, 7)
    events_in = load(events_hbm, events_ref, 0)
    own_q = load(cand_hbm, queries.at[p], 1)
    keys_in = load(keys_hbm, keys_ref, 2)
    values_in = load(values_hbm, values_ref, 3)
    weights_in = [load(w_key_hbm, weight_ref.at[0], 4), load(w_value_hbm, weight_ref.at[1], 5)]
    scalars_in = [load(hist_hbm, hist_ref, 8), load(active_hbm, active_ref, 9)]

    barrier = pltpu.get_barrier_semaphore()
    for peer in (near, far):
        pl.semaphore_signal(barrier, inc=1, device_id={"pos": peer}, device_id_type=MESH)
    for peer in peers:
        @pl.when(peer != me)
        def _():
            pl.semaphore_signal(barrier, inc=1, device_id={"user": peer}, device_id_type=MESH)

    owners_in.wait()
    per_event = events_ref.shape[0]
    features = events_ref.shape[1]
    users = groups * users_here
    owner = owners_ref[...]
    user_id = lax.broadcasted_iota(jnp.int32, (users, per_event), 0)
    same = (user_id == owner).astype(jnp.float32)
    before = (
        lax.broadcasted_iota(jnp.int32, (per_event, per_event), 0)
        <= lax.broadcasted_iota(jnp.int32, (per_event, per_event), 1)
    ).astype(jnp.float32).astype(jnp.bfloat16)
    ranks = jnp.dot(same.astype(jnp.bfloat16), before, preferred_element_type=jnp.float32)
    counts = jnp.sum(same, axis=1, keepdims=True)
    dest = owner // users_here
    earlier = (user_id >= dest * users_here) & (user_id < owner)
    slot = jnp.sum(jnp.where(earlier, counts, 0.0) + same * ranks, axis=0, keepdims=True) - 1.0
    slot = slot.astype(jnp.int32)
    slot_id = lax.broadcasted_iota(jnp.int32, (cap, per_event), 0)
    lane = lax.broadcasted_iota(jnp.int32, (users, features), 1)
    lane_user = lax.broadcasted_iota(jnp.int32, (users, features), 0)

    def hop(ref_src, ref_dst, send, recv, peer):
        return pltpu.make_async_remote_copy(
            src_ref=ref_src, dst_ref=ref_dst, send_sem=send, recv_sem=recv,
            device_id={"pos": peer}, device_id_type=MESH,
        )

    def q_hop(n, c, u, peer):
        return hop(queries.at[c, u], queries.at[c, u], q_send.at[n, u], q_recv.at[n, u], peer)

    def a2a(k):
        return pltpu.make_async_remote_copy(
            src_ref=packed.at[k], dst_ref=rows_ref.at[me],
            send_sem=a2a_send.at[k], recv_sem=a2a_recv.at[k],
            device_id={"user": peers[k]}, device_id_type=MESH,
        )

    def own(k):
        return pltpu.make_async_copy(packed.at[k], rows_ref.at[me], load_sem.at[6])

    def choose(k):
        wanted = jnp.where(dest == peers[k], slot, -1)
        return (wanted == slot_id).astype(jnp.float32).astype(jnp.bfloat16)

    def pack(k, pick):
        peer = peers[k]
        packed[k, :cap, :] = jnp.dot(
            pick, events_ref[...], preferred_element_type=jnp.float32
        ).astype(jnp.bfloat16)
        row = jnp.sum(
            jnp.where(lane_user == lane + peer * users_here, counts, 0.0), axis=0, keepdims=True
        )
        packed[k, cap:, :] = jnp.broadcast_to(row, (TAIL, features)).astype(jnp.bfloat16)

    def post(k):
        @pl.when(peers[k] != me)
        def _():
            a2a(k).start()

        if k == 0:
            @pl.when(peers[k] == me)
            def _():
                own(k).start()

    def arrive(k):
        @pl.when(peers[k] != me)
        def _():
            a2a(k).wait_recv()

        if k == 0:
            @pl.when(peers[k] == me)
            def _():
                own(k).wait()

        forward(k, peers[k]).start()

    def forward(k, source):
        block = rows_ref.at[source]
        return hop(block, block, hop_send.at[k], hop_recv.at[k], near)


    events_in.wait()
    sends = list(range(half))
    pick = choose(sends[0])
    for n in range(len(sends) // 4):
        pack(sends[n], pick)
        pick = choose(sends[n + 1])
    own_q.wait()
    pl.semaphore_wait(barrier, 1 + half + low)
    for u in range(users_here):
        q_hop(0, p, u, far).start()
    for u in range(users_here):
        q_hop(1, p, u, near).start()
    for k in sends[: half // 4]:
        post(k)
    for n in range(half // 4, half):
        after = choose(sends[n + 1]) if n + 1 < half else None
        pack(sends[n], pick)
        pick = after
        post(sends[n])

    eye[...] = (
        lax.broadcasted_iota(jnp.int32, (width, width), 0)
        == lax.broadcasted_iota(jnp.int32, (width, width), 1)
    ).astype(jnp.float32).astype(jnp.bfloat16)
    factor = scale * math.log2(math.e)
    position = lax.broadcasted_iota(jnp.int32, (block_rows, quarter), 0)
    keys_in.wait()
    values_in.wait()
    for copy in scalars_in:
        copy.wait()

    def flip(rows):
        return lax.dot_general(
            eye[...], rows, NT, preferred_element_type=jnp.float32
        ).astype(jnp.bfloat16)

    for u in range(users_here):
        flipped[u] = flip(values_ref[u])
    for copy in weights_in:
        copy.wait()
    turned_weight[...] = flip(weight_ref[1])

    def two_rows(top, total):
        return jnp.concatenate(
            [jnp.broadcast_to(top, (4, quarter)), jnp.broadcast_to(total, (4, quarter))], axis=0
        )

    def weigh(scores, floor):
        top = jnp.maximum(jnp.max(scores, axis=0, keepdims=True) * factor, floor)
        expo = jnp.exp2(scores * factor - top)
        return top, jnp.sum(expo, axis=0, keepdims=True), expo.astype(jnp.bfloat16)

    def copies(pairs, send, recv, n, peer):
        return [
            hop(src, dst, send.at[i, n], recv.at[i, n], peer)
            for i, (src, dst) in enumerate(pairs)
        ]

    def near_copies(n, u):
        return copies(
            (
                (near_out.at[n, u], near_part.at[n, u]),
                (stat.at[2 + n, u], near_stat.at[n, u]),
            ),
            near_send, near_recv, n * users_here + u, near,
        )

    def far_copies(u):
        return copies(
            ((far_out.at[u], far_part.at[u]), (far_stat_out.at[u], far_stat.at[u])),
            far_send, far_recv, u, far,
        )

    def merge(top, total, part, other, other_part):
        new_top = jnp.maximum(top, other[0:1])
        mine = jnp.exp2(top - new_top)
        theirs = jnp.exp2(other[0:1] - new_top)
        total = total * mine + other[4:5] * theirs
        return new_top, total, part * mine + other_part.astype(jnp.float32) * theirs

    def send_far(u):
        for copy in near_copies(1, u):
            copy.wait_recv()
        old = stat[1, u]
        top, total, part = merge(
            old[0:1], old[4:5], acc[1, u], near_stat[1, u], near_part[1, u]
        )
        far_out[u] = part.astype(jnp.bfloat16)
        far_stat_out[u] = two_rows(top, total)
        for copy in far_copies(u):
            copy.start()

    chunk = (p, far, near, cross)

    def ready(kind, u):
        if kind == 2:
            q_hop(1, near, u, near).wait_recv()
        if kind == 1:
            q_hop(0, far, u, far).wait_recv()
            q_hop(2, far, u, near).start()
        if kind == 3:
            q_hop(2, cross, u, near).wait_recv()
            for k in soon[u * len(soon) // users_here : (u + 1) * len(soon) // users_here]:
                arrive(k)

    def finish(kind, u, scores):
        top, total, weights = weigh(
            jnp.where(position < hist_ref[u] - p * block_rows, scores, -1e33), -1e29
        )
        part = jnp.dot(flipped[u], weights, preferred_element_type=jnp.float32)
        stat[kind, u] = two_rows(top, total)
        if kind < 2:
            acc[kind, u] = part
        else:
            near_out[kind - 2, u] = part.astype(jnp.bfloat16)
            for copy in near_copies(kind - 2, u):
                copy.start()
        if kind == 1 and u > 0:
            send_far(u - 1)

    items = [(0, u) for u in range(users_here)]
    for u in range(users_here):
        items += [(2, u)] * (u < users_here - 1) + [(1, u), (3, u)]
    items.append((2, users_here - 1))
    last = None
    for kind, u in items:
        ready(kind, u)
        scores = lax.dot_general(
            keys_ref[u], queries[chunk[kind], u], NT, preferred_element_type=jnp.float32
        )
        if last is not None:
            finish(*last)
        last = (kind, u, scores)
    slots = lax.broadcasted_iota(jnp.int32, (cap, quarter), 0).astype(jnp.float32)

    def project(source):
        raw = rows_ref[source, :cap, :]
        row = pl.multiple_of(STEP + source * cap, 8)
        made = []
        for i in range(2):
            product = jnp.dot(raw, weight_ref[i], preferred_element_type=jnp.float32)
            product = product.astype(jnp.bfloat16)
            made.append(product)
            for n in range(width // 128):
                fresh_ref[i * (width // 128) + n, pl.ds(row, cap)] = product[
                    :, n * 128 : n * 128 + 128
                ].astype(jnp.float32)
        tail = rows_ref[source, cap:, :].astype(jnp.float32)
        begin = jnp.zeros((1, 1), jnp.float32)
        mask = []
        for u in range(users_here):
            end = begin + tail[0:1, u : u + 1]
            mask.append((slots >= begin) & (slots < end))
            begin = end
        turned = lax.dot_general(
            turned_weight[...], raw, NT, preferred_element_type=jnp.float32
        ).astype(jnp.bfloat16)
        return made[0], turned, mask

    def gather(sources, before=()):
        blocks = list(before) + [project(source) for source in sources]
        masks = [
            jnp.concatenate([b[2][u] for b in blocks], axis=0) for u in range(users_here)
        ]
        return (
            jnp.concatenate([b[0] for b in blocks], axis=0),
            jnp.concatenate([b[1] for b in blocks], axis=1),
            masks,
        )

    def score(u, new):
        return lax.dot_general(new[0], queries[p, u], NT, preferred_element_type=jnp.float32)

    def attend(u, new, scores):
        old = stat[0, u]
        top, total, weights = weigh(jnp.where(new[2][u], scores, -1e33), old[0:1])
        shrink = jnp.exp2(old[0:1] - top)
        acc[0, u] = acc[0, u] * shrink + jnp.dot(
            new[1], weights, preferred_element_type=jnp.float32
        )
        stat[0, u] = two_rows(top, total + old[4:5] * shrink)

    def attend_all(new):
        scores = [score(u, new) for u in range(users_here)]
        for u in range(users_here):
            attend(u, new, scores[u])

    for k in soon:
        forward(k, near_sources[k]).wait_recv()
    new = gather([source for k in soon for source in (peers[k], near_sources[k])])
    finish(*last)
    send_far(users_here - 1)
    scores = score(0, new)
    for u in range(users_here):
        after = score(u + 1, new) if u + 1 < users_here else None
        attend(u, new, scores)
        scores = after
        if u == 0:
            for k in mid:
                arrive(k)
            mine = [project(peers[k]) for k in mid]
    for u in range(users_here):
        for copy in near_copies(0, u):
            copy.wait_recv()
    for u in range(users_here):
        old = stat[0, u]
        top, total, part = merge(
            old[0:1], old[4:5], acc[0, u], near_stat[0, u], near_part[0, u]
        )
        acc[0, u] = part
        stat[0, u] = two_rows(top, total)
    for k in mid:
        forward(k, near_sources[k]).wait_recv()
    attend_all(gather([near_sources[k] for k in mid], mine))
    for k in late:
        arrive(k)
    attend_all(gather([peers[k] for k in late]))
    for k in late:
        forward(k, near_sources[k]).wait_recv()
    attend_all(gather([near_sources[k] for k in late]))
    for g in range(groups):
        counts_ref[g : g + 1, :] = rows_ref[g, cap : cap + TAIL, :128].astype(jnp.float32)[
            0:1
        ].astype(jnp.int32)

    for u in range(users_here):
        for copy in far_copies(u):
            copy.wait_recv()
        mine = stat[0, u]
        top, total, part = merge(mine[0:1], mine[4:5], acc[0, u], far_stat[u], far_part[u])
        flag = active_ref[u].astype(jnp.float32)
        out_ref[u] = (part * (flag / total)).T.astype(jnp.bfloat16)
    for u in range(users_here):
        q_hop(0, p, u, far).wait_send()
        q_hop(1, p, u, near).wait_send()
        q_hop(2, far, u, near).wait_send()
        for n in range(2):
            for copy in near_copies(n, u):
                copy.wait_send()
        for copy in far_copies(u):
            copy.wait_send()
    for k in range(half):
        @pl.when(peers[k] != me)
        def _():
            a2a(k).wait_send()

        forward(k, peers[k]).wait_send()


def place_kernel(
    groups, cap,
    count_ref, hist_ref, made_ref, keys_ref, values_ref, attended_ref,
    new_keys_hbm, new_values_hbm, out_hbm,
    cache, out_sem, read_sem,
):
    users_here, rows, width = keys_ref.shape
    sources = (keys_ref, values_ref)
    targets = (new_keys_hbm, new_values_hbm)
    origin = lax.axis_index("pos") * rows
    read = pltpu.make_async_copy(attended_ref, out_hbm, read_sem)
    read.start()

    def leave(u, i, source):
        return pltpu.make_async_copy(source, targets[i].at[u], out_sem.at[u, i])

    begin = [hist_ref[u] - origin for u in range(users_here)]
    end = [
        lax.fori_loop(0, groups, lambda g, n, u=u: n + count_ref[g, u], begin[u])
        for u in range(users_here)
    ]
    touched = [
        (begin[u] < rows) & (end[u] > 0) & (end[u] > begin[u]) for u in range(users_here)
    ]
    for u in range(users_here):
        @pl.when(jnp.logical_not(touched[u]))
        def _():
            for i in range(2):
                leave(u, i, sources[i].at[u]).start()

    row = lax.broadcasted_iota(jnp.int32, (STEP, 128), 0)
    for u in range(users_here):
        @pl.when(touched[u])
        def _():
            for i in range(2):
                cache[u, i] = sources[i][u]

            def place(g, at):
                size = count_ref[g, u]

                @pl.when((size > 0) & (at < rows) & (at + size > 0))
                def _():
                    low = lax.fori_loop(0, u, lambda v, n: n + count_ref[g, v], 0)
                    first = jnp.maximum(at, 0) // 16 * 16
                    last = jnp.minimum(at + size, rows)

                    def blend(n, carry):
                        to = pl.multiple_of(jnp.minimum(first + n * STEP, rows - STEP), 16)
                        start = STEP + g * cap + low + to - at
                        inside = (row >= at - to) & (row < at + size - to)
                        for i in range(2):
                            for tile in range(width // 128):
                                lanes = slice(tile * 128, tile * 128 + 128)
                                fresh = made_ref[i * (width // 128) + tile, pl.ds(start, STEP), :]
                                old = cache[u, i, pl.ds(to, STEP), lanes].astype(jnp.float32)
                                cache[u, i, pl.ds(to, STEP), lanes] = jnp.where(
                                    inside, fresh, old
                                ).astype(jnp.bfloat16)
                        return carry

                    lax.fori_loop(0, (last - first + STEP - 1) // STEP, blend, 0)

                return at + size

            lax.fori_loop(0, groups, place, begin[u])
            for i in range(2):
                leave(u, i, cache.at[u, i]).start()

    for u in range(users_here):
        for i in range(2):
            leave(u, i, sources[i].at[u]).wait()
    read.wait()


def on_device(
    events, owners, offsets, w_key, w_value, cache_keys, cache_values, hist_len, active, candidates
):
    groups = lax.axis_size("user")
    blocks = lax.axis_size("pos")
    users_here, block_rows, width = cache_keys.shape
    per_event, features = events.shape
    cap = 2 * per_event // groups
    quarter = candidates.shape[1]
    half = groups // 2
    vmem = pl.BlockSpec(memory_space=pltpu.VMEM)
    smem = pl.BlockSpec(memory_space=pltpu.SMEM)
    hbm = pl.BlockSpec(memory_space=pltpu.HBM)
    dma = pltpu.SemaphoreType.DMA
    bf16, f32 = jnp.bfloat16, jnp.float32

    made, counts, attended, keys, values = pl.pallas_call(
        functools.partial(merged_kernel, groups, users_here, cap, width ** -0.5),
        out_shape=(
            jax.ShapeDtypeStruct((width // 64, groups * cap + 2 * STEP, 128), f32),
            jax.ShapeDtypeStruct((groups, 128), jnp.int32),
            jax.ShapeDtypeStruct(candidates.shape, bf16),
            jax.ShapeDtypeStruct(cache_keys.shape, bf16),
            jax.ShapeDtypeStruct(cache_values.shape, bf16),
        ),
        in_specs=[hbm] * 9,
        out_specs=(vmem,) * 5,
        scratch_shapes=[
            pltpu.VMEM((1, per_event), jnp.int32),
            pltpu.SMEM(hist_len.shape, jnp.int32),
            pltpu.SMEM(active.shape, jnp.int32),
            pltpu.VMEM(events.shape, bf16),
            pltpu.VMEM((blocks,) + candidates.shape, bf16),
            pltpu.VMEM((2, features, width), bf16),
            pltpu.VMEM((groups, cap + TAIL, features), bf16),
            pltpu.VMEM((half, cap + TAIL, features), bf16),
            pltpu.VMEM((users_here, width, block_rows), bf16),
            pltpu.VMEM((width, width), bf16),
            pltpu.VMEM((width, features), bf16),
            pltpu.VMEM((2, users_here, width, quarter), f32),
            pltpu.VMEM((4, users_here, 8, quarter), f32),
            pltpu.VMEM((2, users_here, width, quarter), bf16),
            pltpu.VMEM((2, users_here, width, quarter), bf16),
            pltpu.VMEM((2, users_here, 8, quarter), f32),
            pltpu.VMEM((users_here, width, quarter), bf16),
            pltpu.VMEM((users_here, 8, quarter), f32),
            pltpu.VMEM((users_here, width, quarter), bf16),
            pltpu.VMEM((users_here, 8, quarter), f32),
            dma((10,)), dma((half,)), dma((half,)), dma((half,)), dma((half,)),
            dma((3, users_here)), dma((3, users_here)),
            dma((2, 2 * users_here)), dma((2, 2 * users_here)),
            dma((2, users_here)), dma((2, users_here)),
        ],
        compiler_params=pltpu.CompilerParams(
            collective_id=0, has_side_effects=True, vmem_limit_bytes=28 * 2**20
        ),
        name="merged",
    )(
        *[
            pltpu.with_memory_space_constraint(x, pltpu.HBM)
            for x in (
                owners.reshape(1, per_event), hist_len, active, events, candidates,
                cache_keys, cache_values, w_key, w_value,
            )
        ]
    )

    return pl.pallas_call(
        functools.partial(place_kernel, groups, cap),
        out_shape=(
            jax.ShapeDtypeStruct(cache_keys.shape, bf16),
            jax.ShapeDtypeStruct(cache_values.shape, bf16),
            jax.ShapeDtypeStruct(candidates.shape, bf16),
        ),
        in_specs=[smem, smem] + [vmem] * 4,
        out_specs=(hbm,) * 3,
        scratch_shapes=[
            pltpu.VMEM((users_here, 2, block_rows, width), bf16),
            dma((users_here, 2)), dma,
        ],
        compiler_params=pltpu.CompilerParams(vmem_limit_bytes=28 * 2**20),
        name="place",
    )(counts, hist_len, made, keys, values, attended)


def solution(mesh):
    placed = (
        P("user", None),
        P("user"),
        P("user"),
        P(),
        P(),
        P("user", "pos", None),
        P("user", "pos", None),
        P("user"),
        P("user"),
        P("user", "pos", None),
    )
    return jax.shard_map(
        on_device,
        mesh=mesh,
        in_specs=placed,
        out_specs=(P("user", "pos", None), P("user", "pos", None), P("user", "pos", None)),
        check_vma=False,
    )
```

```python
import functools
import math

import jax
import jax.numpy as jnp
from jax import lax
from jax.experimental import pallas as pl
from jax.experimental.pallas import tpu as pltpu
from jax.sharding import PartitionSpec as P

MESH = pl.DeviceIdType.MESH
NT = (((1,), (1,)), ((), ()))
TAIL = 16
STEP = 64


def pos_peers():
    p = lax.axis_index("pos")
    near = p + 1 - 2 * lax.rem(p, 2)
    far = lax.rem(p + 2, 4)
    return p, near, far


def merged_kernel(
    groups, users_here, cap, scale,
    owners_hbm, hist_hbm, active_hbm, events_hbm, cand_hbm, keys_hbm, values_hbm,
    w_key_hbm, w_value_hbm,
    fresh_ref, counts_ref, out_ref, keys_ref, values_ref,
    owners_ref, hist_ref, active_ref, events_ref, queries, weight_ref, rows_ref, packed, flipped, eye, turned_weight,
    acc, stat, near_out, near_part, near_stat, far_out, far_stat_out, far_part, far_stat,
    load_sem, a2a_send, a2a_recv, hop_send, hop_recv, q_send, q_recv,
    near_send, near_recv, far_send, far_recv,
):
    me = lax.axis_index("user")
    p, near, far = pos_peers()
    low, high = lax.rem(p, 2), p // 2
    cross = 2 * (1 - high) + 1 - low
    half = groups // 2

    def partner(k, odd):
        bit = lax.rem(me, 2)
        there = me + odd * (1 - 2 * bit)
        for n in range(1, groups.bit_length() - 1):
            if (2 * k >> n) % 2:
                there += (1 - 2 * lax.rem(me // 2**n, 2)) * 2**n
        return there

    peers = [partner(k, low) for k in range(half)]
    near_sources = [partner(k, 1 - low) for k in range(half)]
    soon, mid, late = range(half // 2), range(half // 2, 3 * half // 4), range(3 * half // 4, half)
    block_rows, width = keys_ref.shape[1:]
    quarter = queries.shape[2]

    def load(src, dst, n):
        copy = pltpu.make_async_copy(src, dst, load_sem.at[n])
        copy.start()
        return copy

    owners_in = load(owners_hbm, owners_ref, 7)
    events_in = load(events_hbm, events_ref, 0)
    own_q = load(cand_hbm, queries.at[p], 1)
    keys_in = load(keys_hbm, keys_ref, 2)
    values_in = load(values_hbm, values_ref, 3)
    weights_in = [load(w_key_hbm, weight_ref.at[0], 4), load(w_value_hbm, weight_ref.at[1], 5)]
    scalars_in = [load(hist_hbm, hist_ref, 8), load(active_hbm, active_ref, 9)]

    barrier = pltpu.get_barrier_semaphore()
    for peer in (near, far):
        pl.semaphore_signal(barrier, inc=1, device_id={"pos": peer}, device_id_type=MESH)
    for peer in peers:
        @pl.when(peer != me)
        def _():
            pl.semaphore_signal(barrier, inc=1, device_id={"user": peer}, device_id_type=MESH)

    owners_in.wait()
    per_event = events_ref.shape[0]
    features = events_ref.shape[1]
    users = groups * users_here
    owner = owners_ref[...]
    user_id = lax.broadcasted_iota(jnp.int32, (users, per_event), 0)
    same = (user_id == owner).astype(jnp.float32)
    before = (
        lax.broadcasted_iota(jnp.int32, (per_event, per_event), 0)
        <= lax.broadcasted_iota(jnp.int32, (per_event, per_event), 1)
    ).astype(jnp.float32).astype(jnp.bfloat16)
    ranks = jnp.dot(same.astype(jnp.bfloat16), before, preferred_element_type=jnp.float32)
    counts = jnp.sum(same, axis=1, keepdims=True)
    dest = owner // users_here
    earlier = (user_id >= dest * users_here) & (user_id < owner)
    slot = jnp.sum(jnp.where(earlier, counts, 0.0) + same * ranks, axis=0, keepdims=True) - 1.0
    slot = slot.astype(jnp.int32)
    slot_id = lax.broadcasted_iota(jnp.int32, (cap, per_event), 0)
    lane = lax.broadcasted_iota(jnp.int32, (users, features), 1)
    lane_user = lax.broadcasted_iota(jnp.int32, (users, features), 0)

    def hop(ref_src, ref_dst, send, recv, peer):
        return pltpu.make_async_remote_copy(
            src_ref=ref_src, dst_ref=ref_dst, send_sem=send, recv_sem=recv,
            device_id={"pos": peer}, device_id_type=MESH,
        )

    def q_hop(n, c, u, peer):
        return hop(queries.at[c, u], queries.at[c, u], q_send.at[n, u], q_recv.at[n, u], peer)

    def a2a(k):
        return pltpu.make_async_remote_copy(
            src_ref=packed.at[k], dst_ref=rows_ref.at[me],
            send_sem=a2a_send.at[k], recv_sem=a2a_recv.at[k],
            device_id={"user": peers[k]}, device_id_type=MESH,
        )

    def own(k):
        return pltpu.make_async_copy(packed.at[k], rows_ref.at[me], load_sem.at[6])

    def choose(k):
        wanted = jnp.where(dest == peers[k], slot, -1)
        return (wanted == slot_id).astype(jnp.float32).astype(jnp.bfloat16)

    def pack(k, pick):
        peer = peers[k]
        packed[k, :cap, :] = jnp.dot(
            pick, events_ref[...], preferred_element_type=jnp.float32
        ).astype(jnp.bfloat16)
        row = jnp.sum(
            jnp.where(lane_user == lane + peer * users_here, counts, 0.0), axis=0, keepdims=True
        )
        packed[k, cap:, :] = jnp.broadcast_to(row, (TAIL, features)).astype(jnp.bfloat16)

    def post(k):
        @pl.when(peers[k] != me)
        def _():
            a2a(k).start()

        if k == 0:
            @pl.when(peers[k] == me)
            def _():
                own(k).start()

    def arrive(k):
        @pl.when(peers[k] != me)
        def _():
            a2a(k).wait_recv()

        if k == 0:
            @pl.when(peers[k] == me)
            def _():
                own(k).wait()

        forward(k, peers[k]).start()

    def forward(k, source):
        block = rows_ref.at[source]
        return hop(block, block, hop_send.at[k], hop_recv.at[k], near)


    events_in.wait()
    sends = list(range(half))
    pick = choose(sends[0])
    for n in range(len(sends) // 4):
        pack(sends[n], pick)
        pick = choose(sends[n + 1])
    own_q.wait()
    pl.semaphore_wait(barrier, 1 + half + low)
    for u in range(users_here):
        q_hop(0, p, u, far).start()
    for u in range(users_here):
        q_hop(1, p, u, near).start()
    for k in sends[: half // 4]:
        post(k)
    for n in range(half // 4, half):
        after = choose(sends[n + 1]) if n + 1 < half else None
        pack(sends[n], pick)
        pick = after
        post(sends[n])

    eye[...] = (
        lax.broadcasted_iota(jnp.int32, (width, width), 0)
        == lax.broadcasted_iota(jnp.int32, (width, width), 1)
    ).astype(jnp.float32).astype(jnp.bfloat16)
    factor = scale * math.log2(math.e)
    position = lax.broadcasted_iota(jnp.int32, (block_rows, quarter), 0)
    keys_in.wait()
    values_in.wait()
    for copy in scalars_in:
        copy.wait()

    def flip(rows):
        return lax.dot_general(
            eye[...], rows, NT, preferred_element_type=jnp.float32
        ).astype(jnp.bfloat16)

    for u in range(users_here):
        flipped[u] = flip(values_ref[u])
    for copy in weights_in:
        copy.wait()
    turned_weight[...] = flip(weight_ref[1])

    def two_rows(top, total):
        return jnp.concatenate(
            [jnp.broadcast_to(top, (4, quarter)), jnp.broadcast_to(total, (4, quarter))], axis=0
        )

    def weigh(scores, floor):
        top = jnp.maximum(jnp.max(scores, axis=0, keepdims=True) * factor, floor)
        expo = jnp.exp2(scores * factor - top)
        return top, jnp.sum(expo, axis=0, keepdims=True), expo.astype(jnp.bfloat16)

    def copies(pairs, send, recv, n, peer):
        return [
            hop(src, dst, send.at[i, n], recv.at[i, n], peer)
            for i, (src, dst) in enumerate(pairs)
        ]

    def near_copies(n, u):
        return copies(
            (
                (near_out.at[n, u], near_part.at[n, u]),
                (stat.at[2 + n, u], near_stat.at[n, u]),
            ),
            near_send, near_recv, n * users_here + u, near,
        )

    def far_copies(u):
        return copies(
            ((far_out.at[u], far_part.at[u]), (far_stat_out.at[u], far_stat.at[u])),
            far_send, far_recv, u, far,
        )

    def merge(top, total, part, other, other_part):
        new_top = jnp.maximum(top, other[0:1])
        mine = jnp.exp2(top - new_top)
        theirs = jnp.exp2(other[0:1] - new_top)
        total = total * mine + other[4:5] * theirs
        return new_top, total, part * mine + other_part.astype(jnp.float32) * theirs

    def send_far(u):
        for copy in near_copies(1, u):
            copy.wait_recv()
        old = stat[1, u]
        top, total, part = merge(
            old[0:1], old[4:5], acc[1, u], near_stat[1, u], near_part[1, u]
        )
        far_out[u] = part.astype(jnp.bfloat16)
        far_stat_out[u] = two_rows(top, total)
        for copy in far_copies(u):
            copy.start()

    chunk = (p, far, near, cross)

    def ready(kind, u):
        if kind == 2:
            q_hop(1, near, u, near).wait_recv()
        if kind == 1:
            q_hop(0, far, u, far).wait_recv()
            q_hop(2, far, u, near).start()
        if kind == 3:
            q_hop(2, cross, u, near).wait_recv()
            for k in soon[u * len(soon) // users_here : (u + 1) * len(soon) // users_here]:
                arrive(k)

    def finish(kind, u, scores):
        top, total, weights = weigh(
            jnp.where(position < hist_ref[u] - p * block_rows, scores, -1e33), -1e29
        )
        part = jnp.dot(flipped[u], weights, preferred_element_type=jnp.float32)
        stat[kind, u] = two_rows(top, total)
        if kind < 2:
            acc[kind, u] = part
        else:
            near_out[kind - 2, u] = part.astype(jnp.bfloat16)
            for copy in near_copies(kind - 2, u):
                copy.start()
        if kind == 1 and u > 0:
            send_far(u - 1)

    items = [(0, u) for u in range(users_here)]
    for u in range(users_here):
        items += [(2, u)] * (u < users_here - 1) + [(1, u), (3, u)]
    items.append((2, users_here - 1))
    last = None
    for kind, u in items:
        ready(kind, u)
        scores = lax.dot_general(
            keys_ref[u], queries[chunk[kind], u], NT, preferred_element_type=jnp.float32
        )
        if last is not None:
            finish(*last)
        last = (kind, u, scores)
    slots = lax.broadcasted_iota(jnp.int32, (cap, quarter), 0).astype(jnp.float32)

    def project(source):
        raw = rows_ref[source, :cap, :]
        row = pl.multiple_of(STEP + source * cap, 8)
        made = []
        for i in range(2):
            product = jnp.dot(raw, weight_ref[i], preferred_element_type=jnp.float32)
            product = product.astype(jnp.bfloat16)
            made.append(product)
            for n in range(width // 128):
                fresh_ref[i * (width // 128) + n, pl.ds(row, cap)] = product[
                    :, n * 128 : n * 128 + 128
                ].astype(jnp.float32)
        tail = rows_ref[source, cap:, :].astype(jnp.float32)
        begin = jnp.zeros((1, 1), jnp.float32)
        mask = []
        for u in range(users_here):
            end = begin + tail[0:1, u : u + 1]
            mask.append((slots >= begin) & (slots < end))
            begin = end
        turned = lax.dot_general(
            turned_weight[...], raw, NT, preferred_element_type=jnp.float32
        ).astype(jnp.bfloat16)
        return made[0], turned, mask

    def gather(sources, before=()):
        blocks = list(before) + [project(source) for source in sources]
        masks = [
            jnp.concatenate([b[2][u] for b in blocks], axis=0) for u in range(users_here)
        ]
        return (
            jnp.concatenate([b[0] for b in blocks], axis=0),
            jnp.concatenate([b[1] for b in blocks], axis=1),
            masks,
        )

    def score(u, new):
        return lax.dot_general(new[0], queries[p, u], NT, preferred_element_type=jnp.float32)

    def attend(u, new, scores):
        old = stat[0, u]
        top, total, weights = weigh(jnp.where(new[2][u], scores, -1e33), old[0:1])
        shrink = jnp.exp2(old[0:1] - top)
        acc[0, u] = acc[0, u] * shrink + jnp.dot(
            new[1], weights, preferred_element_type=jnp.float32
        )
        stat[0, u] = two_rows(top, total + old[4:5] * shrink)

    def attend_all(new):
        scores = [score(u, new) for u in range(users_here)]
        for u in range(users_here):
            attend(u, new, scores[u])

    for k in soon:
        forward(k, near_sources[k]).wait_recv()
    new = gather([source for k in soon for source in (peers[k], near_sources[k])])
    finish(*last)
    scores = score(0, new)
    for u in range(users_here):
        after = score(u + 1, new) if u + 1 < users_here else None
        attend(u, new, scores)
        scores = after
        if u == 0:
            send_far(users_here - 1)
            for k in mid:
                arrive(k)
            mine = [project(peers[k]) for k in mid]
    for u in range(users_here):
        for copy in near_copies(0, u):
            copy.wait_recv()
    for u in range(users_here):
        old = stat[0, u]
        top, total, part = merge(
            old[0:1], old[4:5], acc[0, u], near_stat[0, u], near_part[0, u]
        )
        acc[0, u] = part
        stat[0, u] = two_rows(top, total)
    for k in mid:
        forward(k, near_sources[k]).wait_recv()
    attend_all(gather([near_sources[k] for k in mid], mine))
    for k in late:
        arrive(k)
    attend_all(gather([peers[k] for k in late]))
    for k in late:
        forward(k, near_sources[k]).wait_recv()
    attend_all(gather([near_sources[k] for k in late]))
    for g in range(groups):
        counts_ref[g : g + 1, :] = rows_ref[g, cap : cap + TAIL, :128].astype(jnp.float32)[
            0:1
        ].astype(jnp.int32)

    for u in range(users_here):
        for copy in far_copies(u):
            copy.wait_recv()
        mine = stat[0, u]
        top, total, part = merge(mine[0:1], mine[4:5], acc[0, u], far_stat[u], far_part[u])
        flag = active_ref[u].astype(jnp.float32)
        out_ref[u] = (part * (flag / total)).T.astype(jnp.bfloat16)
    for u in range(users_here):
        q_hop(0, p, u, far).wait_send()
        q_hop(1, p, u, near).wait_send()
        q_hop(2, far, u, near).wait_send()
        for n in range(2):
            for copy in near_copies(n, u):
                copy.wait_send()
        for copy in far_copies(u):
            copy.wait_send()
    for k in range(half):
        @pl.when(peers[k] != me)
        def _():
            a2a(k).wait_send()

        forward(k, peers[k]).wait_send()


def place_kernel(
    groups, cap,
    count_ref, hist_ref, made_ref, keys_ref, values_ref, attended_ref,
    new_keys_hbm, new_values_hbm, out_hbm,
    cache, out_sem, read_sem,
):
    users_here, rows, width = keys_ref.shape
    sources = (keys_ref, values_ref)
    targets = (new_keys_hbm, new_values_hbm)
    origin = lax.axis_index("pos") * rows
    read = pltpu.make_async_copy(attended_ref, out_hbm, read_sem)
    read.start()

    def leave(u, i, source):
        return pltpu.make_async_copy(source, targets[i].at[u], out_sem.at[u, i])

    begin = [hist_ref[u] - origin for u in range(users_here)]
    end = [
        lax.fori_loop(0, groups, lambda g, n, u=u: n + count_ref[g, u], begin[u])
        for u in range(users_here)
    ]
    touched = [
        (begin[u] < rows) & (end[u] > 0) & (end[u] > begin[u]) for u in range(users_here)
    ]
    for u in range(users_here):
        @pl.when(jnp.logical_not(touched[u]))
        def _():
            for i in range(2):
                leave(u, i, sources[i].at[u]).start()

    row = lax.broadcasted_iota(jnp.int32, (STEP, 128), 0)
    for u in range(users_here):
        @pl.when(touched[u])
        def _():
            for i in range(2):
                cache[u, i] = sources[i][u]

            def place(g, at):
                size = count_ref[g, u]

                @pl.when((size > 0) & (at < rows) & (at + size > 0))
                def _():
                    low = lax.fori_loop(0, u, lambda v, n: n + count_ref[g, v], 0)
                    first = jnp.maximum(at, 0) // 16 * 16
                    last = jnp.minimum(at + size, rows)

                    def blend(n, carry):
                        to = pl.multiple_of(jnp.minimum(first + n * STEP, rows - STEP), 16)
                        start = STEP + g * cap + low + to - at
                        inside = (row >= at - to) & (row < at + size - to)
                        for i in range(2):
                            for tile in range(width // 128):
                                lanes = slice(tile * 128, tile * 128 + 128)
                                fresh = made_ref[i * (width // 128) + tile, pl.ds(start, STEP), :]
                                old = cache[u, i, pl.ds(to, STEP), lanes].astype(jnp.float32)
                                cache[u, i, pl.ds(to, STEP), lanes] = jnp.where(
                                    inside, fresh, old
                                ).astype(jnp.bfloat16)
                        return carry

                    lax.fori_loop(0, (last - first + STEP - 1) // STEP, blend, 0)

                return at + size

            lax.fori_loop(0, groups, place, begin[u])
            for i in range(2):
                leave(u, i, cache.at[u, i]).start()

    for u in range(users_here):
        for i in range(2):
            leave(u, i, sources[i].at[u]).wait()
    read.wait()


def on_device(
    events, owners, offsets, w_key, w_value, cache_keys, cache_values, hist_len, active, candidates
):
    groups = lax.axis_size("user")
    blocks = lax.axis_size("pos")
    users_here, block_rows, width = cache_keys.shape
    per_event, features = events.shape
    cap = 2 * per_event // groups
    quarter = candidates.shape[1]
    half = groups // 2
    vmem = pl.BlockSpec(memory_space=pltpu.VMEM)
    smem = pl.BlockSpec(memory_space=pltpu.SMEM)
    hbm = pl.BlockSpec(memory_space=pltpu.HBM)
    dma = pltpu.SemaphoreType.DMA
    bf16, f32 = jnp.bfloat16, jnp.float32

    made, counts, attended, keys, values = pl.pallas_call(
        functools.partial(merged_kernel, groups, users_here, cap, width ** -0.5),
        out_shape=(
            jax.ShapeDtypeStruct((width // 64, groups * cap + 2 * STEP, 128), f32),
            jax.ShapeDtypeStruct((groups, 128), jnp.int32),
            jax.ShapeDtypeStruct(candidates.shape, bf16),
            jax.ShapeDtypeStruct(cache_keys.shape, bf16),
            jax.ShapeDtypeStruct(cache_values.shape, bf16),
        ),
        in_specs=[hbm] * 9,
        out_specs=(vmem,) * 5,
        scratch_shapes=[
            pltpu.VMEM((1, per_event), jnp.int32),
            pltpu.SMEM(hist_len.shape, jnp.int32),
            pltpu.SMEM(active.shape, jnp.int32),
            pltpu.VMEM(events.shape, bf16),
            pltpu.VMEM((blocks,) + candidates.shape, bf16),
            pltpu.VMEM((2, features, width), bf16),
            pltpu.VMEM((groups, cap + TAIL, features), bf16),
            pltpu.VMEM((half, cap + TAIL, features), bf16),
            pltpu.VMEM((users_here, width, block_rows), bf16),
            pltpu.VMEM((width, width), bf16),
            pltpu.VMEM((width, features), bf16),
            pltpu.VMEM((2, users_here, width, quarter), f32),
            pltpu.VMEM((4, users_here, 8, quarter), f32),
            pltpu.VMEM((2, users_here, width, quarter), bf16),
            pltpu.VMEM((2, users_here, width, quarter), bf16),
            pltpu.VMEM((2, users_here, 8, quarter), f32),
            pltpu.VMEM((users_here, width, quarter), bf16),
            pltpu.VMEM((users_here, 8, quarter), f32),
            pltpu.VMEM((users_here, width, quarter), bf16),
            pltpu.VMEM((users_here, 8, quarter), f32),
            dma((10,)), dma((half,)), dma((half,)), dma((half,)), dma((half,)),
            dma((3, users_here)), dma((3, users_here)),
            dma((2, 2 * users_here)), dma((2, 2 * users_here)),
            dma((2, users_here)), dma((2, users_here)),
        ],
        compiler_params=pltpu.CompilerParams(
            collective_id=0, has_side_effects=True, vmem_limit_bytes=28 * 2**20
        ),
        name="merged",
    )(
        *[
            pltpu.with_memory_space_constraint(x, pltpu.HBM)
            for x in (
                owners.reshape(1, per_event), hist_len, active, events, candidates,
                cache_keys, cache_values, w_key, w_value,
            )
        ]
    )

    return pl.pallas_call(
        functools.partial(place_kernel, groups, cap),
        out_shape=(
            jax.ShapeDtypeStruct(cache_keys.shape, bf16),
            jax.ShapeDtypeStruct(cache_values.shape, bf16),
            jax.ShapeDtypeStruct(candidates.shape, bf16),
        ),
        in_specs=[smem, smem] + [vmem] * 4,
        out_specs=(hbm,) * 3,
        scratch_shapes=[
            pltpu.VMEM((users_here, 2, block_rows, width), bf16),
            dma((users_here, 2)), dma,
        ],
        compiler_params=pltpu.CompilerParams(vmem_limit_bytes=28 * 2**20),
        name="place",
    )(counts, hist_len, made, keys, values, attended)


def solution(mesh):
    placed = (
        P("user", None),
        P("user"),
        P("user"),
        P(),
        P(),
        P("user", "pos", None),
        P("user", "pos", None),
        P("user"),
        P("user"),
        P("user", "pos", None),
    )
    return jax.shard_map(
        on_device,
        mesh=mesh,
        in_specs=placed,
        out_specs=(P("user", "pos", None), P("user", "pos", None), P("user", "pos", None)),
        check_vma=False,
    )
```
